32 devices in a mesh: tm: 4 (over y, x), rows: 2 (over core), batch: 4 (over z).
Axes of the slice: x: 2, y: 2, z: 4, core: 2. Of those that a mesh axis runs over, the one named last changes fastest.
Arguments:
- inputs: bfloat16 [4, 8, 16, 128, 384], P('batch', 'tm', 'rows'), parts along dimension 0, may hold values from -16 to 16
- norm_gain: float32 [384], replicated, may hold values from 0.1 to 1.9
- norm_bias: float32 [384], replicated, may hold values from -3 to 3
- conv_weight: bfloat16 [3, 3, 3, 384, 384], replicated, may hold values from -0.0625 to 0.0625
- conv_bias: float32 [384], replicated, may hold values from -2 to 2
Outputs:
- decoded: bfloat16 [4, 8, 16, 128, 384], P('batch', 'tm', 'rows'), parts along dimension 0
The draws below stay inside these ranges and needn't reach their ends.
There are 4 independent parts, one for each index of `batch`. The reference program is written for one: setup_inputs(seed, part) draws one part's arguments, and reference() takes and returns one part's arrays. A program takes and returns all parts, laid end to end along the dimension named above; an argument that names none is the same for every part. Nothing has to cross between parts.
All inputs are finite; a program needn't handle non-finite values.
Results may differ from the reference program's by a relative error of at most 0.0025.
Values may be sent and summed in bfloat16 or wider, within the bound.
No kernel may reach another device: no remote copies, remote signals or barrier semaphores. Data moves between devices by JAX's collectives and lax.ppermute only.
A program may use at most 128 MiB of HBM per device.

```python
import jax
import jax.numpy as jnp
from jax import lax

CHANNELS = 384
GROUPS = 32
WIDTH = 128
CLIPS = 1
FRAMES = 8
HEIGHT = 16


def draw_inputs(key, part):
    subkeys = jax.random.split(jax.random.fold_in(key, 17), 4)
    full_shape = (CLIPS, FRAMES, HEIGHT, WIDTH, CHANNELS)
    scales = 0.6 * jnp.exp(jax.random.uniform(subkeys[0], (CLIPS, FRAMES, HEIGHT, 1, 1), jnp.float32, -1.2, 1.2))
    offsets = 1.2 + 0.4 * jax.random.truncated_normal(subkeys[1], -5.0, 5.0, (CHANNELS,), jnp.float32)
    row_place = (jnp.arange(HEIGHT, dtype=jnp.float32) + 0.5) / HEIGHT
    row_ramp = (3.0 * row_place - 1.5).reshape(1, 1, HEIGHT, 1, 1)
    frame_level = jax.random.uniform(subkeys[3], (CLIPS, FRAMES, 1, 1, 1), jnp.float32, -1.2, 1.2)
    region = row_ramp + frame_level
    noisy_part = jax.random.truncated_normal(subkeys[2], -4.0, 4.0, full_shape, jnp.float32)
    values = noisy_part * scales + offsets + region
    return values.astype(jnp.bfloat16)


def bell_draw(key, extent, scale, limit, kind=jnp.bfloat16):
    values = jax.random.normal(key, extent, jnp.float32) * scale
    return jnp.minimum(jnp.maximum(values, -limit), limit).astype(kind)


def setup_inputs(seed: int = 0, part: int = 0) -> dict:
    key_list = jax.random.split(jax.random.key(seed), 6)
    own_keys = jax.random.split(jax.random.fold_in(key_list[5], part), 6)
    return {
        "inputs": draw_inputs(jax.random.fold_in(jax.random.fold_in(key_list[5], part), 71), part),
        "norm_gain": jnp.clip(1.0 + 0.18 * jax.random.normal(key_list[1], (CHANNELS,), jnp.float32), 0.1, 1.9),
        "norm_bias": bell_draw(key_list[2], (CHANNELS,), 0.5, 3.0, jnp.float32),
        "conv_weight": bell_draw(key_list[3], (3, 3, 3, CHANNELS, CHANNELS), (27 * CHANNELS) ** -0.5, 0.0625),
        "conv_bias": bell_draw(key_list[4], (CHANNELS,), 0.3, 2.0, jnp.float32),
    }


epsilon = 1e-06

def convolve(padded, conv_weight, frames, height, width):
    channels = padded.shape[-1]
    summed = jnp.zeros((padded.shape[0] * frames * height * width, conv_weight.shape[-1]), jnp.float32)
    for tap_time in range(3):
        for tap_row in range(3):
            slab_rows = padded[:, tap_time:tap_time + frames, tap_row:tap_row + height]
            columns = jnp.concatenate([slab_rows[:, :, :, 0:width], slab_rows[:, :, :, 1:width + 1], slab_rows[:, :, :, 2:width + 2]], axis=-1)
            kernel = conv_weight[tap_time, tap_row].reshape(3 * channels, -1)
            summed = summed + jnp.dot(columns.reshape(-1, 3 * channels), kernel, preferred_element_type=jnp.float32)
    return summed

def reference(inputs, norm_gain, norm_bias, conv_weight, conv_bias):
    values = inputs.astype(jnp.float32)
    channels = values.shape[-1]
    per_group = channels // GROUPS
    cell_count = 1.0 * CLIPS * FRAMES * HEIGHT * WIDTH * per_group
    chan_sum = lax.optimization_barrier(jnp.sum(values, axis=(0, 1, 2, 3)))
    group_mean = lax.optimization_barrier(jnp.sum(chan_sum.reshape(GROUPS, per_group), axis=1)) / cell_count
    centered = values - jnp.repeat(group_mean, per_group)
    chan_square = lax.optimization_barrier(jnp.sum(centered * centered, axis=(0, 1, 2, 3)))
    group_var = lax.optimization_barrier(jnp.sum(chan_square.reshape(GROUPS, per_group), axis=1)) / cell_count
    inverse = jnp.repeat(lax.rsqrt(group_var + epsilon), per_group)
    normed = centered * inverse * norm_gain + norm_bias
    active = (normed * jax.nn.sigmoid(normed)).astype(jnp.bfloat16)
    padded = jnp.pad(active, ((0, 0), (2, 0), (1, 1), (1, 1), (0, 0)))
    summed = convolve(padded, conv_weight, FRAMES, HEIGHT, WIDTH)
    result = values + summed.reshape(values.shape) + conv_bias
    return result.astype(jnp.bfloat16)
```

```python
import functools

import jax
import jax.numpy as jnp
from jax import lax
from jax.experimental import pallas as pl
from jax.experimental.pallas import tpu as pltpu
from jax.sharding import PartitionSpec as P

GROUPS = 32
epsilon = 1e-06
TAPS = 3
VMEM_LIMIT = 56 * 1024 * 1024


def ring(value, axis, step):
    count = lax.axis_size(axis)
    return lax.ppermute(value, axis, [(i, (i + step) % count) for i in range(count)])


def row_halo(first, last, axis):
    count = lax.axis_size(axis)
    if count == 1:
        return first, last
    if count == 2:
        both = ring(jnp.where(lax.axis_index(axis) == 0, last, first), axis, 1)
        return both, both
    return ring(last, axis, 1), ring(first, axis, -1)


def merged(stats, axis, count):
    size = lax.axis_size(axis)
    step = 1
    while step < size:
        other = lax.ppermute(stats, axis, [(i, i ^ step) for i in range(size)])
        gap = stats[0:1] - other[0:1]
        extra = gap * gap * (0.5 / count)
        both = stats + other
        stats = jnp.concatenate([both[0:1], both[1:2] + extra], axis=0)
        count = 2.0 * count
        step *= 2
    return stats, count


def stats_kernel(x_ref, out_ref):
    rows, width, channels = x_ref.shape
    total = jnp.zeros((8, channels), jnp.float32)

    def add(r, total):
        return total + jnp.sum(x_ref[r].astype(jnp.float32).reshape(-1, 8, channels), axis=0)

    total = lax.fori_loop(0, rows, add, total, unroll=2)
    chan_sum = jnp.sum(total, axis=0, keepdims=True)
    mean = chan_sum * (1.0 / (rows * width))

    def square(r, total):
        gap = x_ref[r].astype(jnp.float32) - mean
        return total + jnp.sum((gap * gap).reshape(-1, 8, channels), axis=0)

    total = lax.fori_loop(0, rows, square, jnp.zeros((8, channels), jnp.float32), unroll=2)
    out_ref[0:1] = chan_sum
    out_ref[1:2] = jnp.sum(total, axis=0, keepdims=True)


def affine(stats_ref, gain_ref, bias_ref, aff_ref, count):
    channels = stats_ref.shape[-1]
    per_group = channels // GROUPS
    row = lax.broadcasted_iota(jnp.int32, (channels, channels), 0)
    col = lax.broadcasted_iota(jnp.int32, (channels, channels), 1)
    same = jnp.where(row // per_group == col // per_group, 1.0, 0.0)

    def group_mean(v):
        wide = jnp.broadcast_to(v, (8, channels))
        dot = jnp.dot(wide, same, precision=lax.Precision.HIGHEST, preferred_element_type=jnp.float32)
        return dot[0:1] * (1.0 / per_group)

    chan_mean = stats_ref[0:1] * (1.0 / count)
    mean = group_mean(chan_mean)
    gap = chan_mean - mean
    var = group_mean(stats_ref[1:2] * (1.0 / count) + gap * gap)
    aff_ref[0:1] = mean
    aff_ref[1:2] = lax.rsqrt(var + epsilon) * gain_ref[...]
    aff_ref[2:3] = bias_ref[...]


def activate(raw, aff, keep, act_ref, slot):
    width, channels = raw.shape
    normed = (raw.astype(jnp.float32) - aff[0:1]) * aff[1:2] + aff[2:3]
    active = normed * jax.nn.sigmoid(normed)
    active = jnp.where(keep != 0, active, 0.0)
    place = lax.broadcasted_iota(jnp.int32, (width, channels), 0)
    before = jnp.where(place == 0, 0.0, pltpu.roll(active, 1, 0))
    after = jnp.where(place == width - 1, 0.0, pltpu.roll(active, width - 1, 0))
    act_ref[slot, :, 0:channels] = before.astype(jnp.bfloat16)
    act_ref[slot, :, channels : 2 * channels] = active.astype(jnp.bfloat16)
    act_ref[slot, :, 2 * channels : 3 * channels] = after.astype(jnp.bfloat16)


def row_dots(act_ref, first, rows, weight):
    total = None
    for kh in range(TAPS):
        lhs = act_ref[pl.ds(first + kh, rows)]
        lhs = lhs.reshape(-1, lhs.shape[-1])
        part = jnp.dot(lhs, weight(kh), preferred_element_type=jnp.float32)
        total = part if total is None else total + part
    return total


def own_kernel(count, block, flags_ref, x_ref, top_ref, bottom_ref, stats_ref, gain_ref, bias_ref, w_ref,
               acc0_ref, acc1_ref, aff_ref, act0_ref, act1_ref, wide_ref, last_ref, sems):
    frames, height, width, channels = x_ref.shape
    copies = []
    for kh in range(TAPS):
        copies.append(pltpu.make_async_copy(w_ref.at[2, kh], wide_ref.at[kh, :, 0:channels], sems.at[3 * kh]))
        copies.append(pltpu.make_async_copy(w_ref.at[1, kh], wide_ref.at[kh, :, channels : 2 * channels], sems.at[3 * kh + 1]))
        copies.append(pltpu.make_async_copy(w_ref.at[2, kh], last_ref.at[kh], sems.at[3 * kh + 2]))
    for copy in copies:
        copy.start()
    affine(stats_ref, gain_ref, bias_ref, aff_ref, count)
    aff = aff_ref[0:3]
    for f, act_ref in ((0, act0_ref), (1, act1_ref)):
        activate(top_ref[f], aff, flags_ref[1], act_ref, 0)
        activate(bottom_ref[f], aff, flags_ref[2], act_ref, height + 1)
        for r in range(block + 1):
            activate(x_ref[f, r], aff, 1, act_ref, r + 1)
    for copy in copies:
        copy.wait()

    def step(i, _):
        first = i * block
        both = row_dots(act0_ref, first, block, lambda kh: wide_ref[kh])
        last = row_dots(act1_ref, first, block, lambda kh: last_ref[kh])
        acc0_ref[pl.ds(first, block)] = both[:, 0:channels].reshape(block, width, channels)
        acc1_ref[pl.ds(first, block)] = (both[:, channels:] + last).reshape(block, width, channels)
        for r in range(block):
            row = jnp.minimum(first + block + 1 + r, height - 1)
            for f, act_ref in ((0, act0_ref), (1, act1_ref)):
                activate(x_ref[f, row], aff, 1, act_ref, row + 1)
        return 0

    lax.fori_loop(0, height // block, step, 0)


def near_kernel(block, flags_ref, edge_ref, mid_ref, top_ref, bottom_ref, aff_ref, x_ref, cbias_ref, acc0_ref, acc1_ref, w_ref,
                new0_ref, out_ref, act_ref, wide_ref, line_ref, sems):
    height, width, channels = acc0_ref.shape
    copies = []
    for kh in range(TAPS):
        copies.append(pltpu.make_async_copy(w_ref.at[1, kh], wide_ref.at[kh, :, 0:channels], sems.at[2 * kh]))
        copies.append(pltpu.make_async_copy(w_ref.at[0, kh], wide_ref.at[kh, :, channels : 2 * channels], sems.at[2 * kh + 1]))
    for copy in copies:
        copy.start()
    aff = aff_ref[0:3]
    keep = flags_ref[0]
    activate(top_ref[...], aff, keep * flags_ref[1], act_ref, 0)
    activate(bottom_ref[...], aff, keep * flags_ref[2], act_ref, height + 1)
    activate(edge_ref[0], aff, keep, act_ref, 1)
    activate(edge_ref[1], aff, keep, act_ref, height)
    for r in range(1, block + 1):
        activate(mid_ref[r - 1], aff, keep, act_ref, r + 1)
    for copy in copies:
        copy.wait()

    def step(i, _):
        first = i * block
        both = row_dots(act_ref, first, block, lambda kh: wide_ref[kh]).reshape(block, width, 2 * channels)
        here = pl.ds(first, block)
        new0_ref[here] = acc0_ref[here] + both[:, :, 0:channels]
        done = x_ref[here].astype(jnp.float32) + (acc1_ref[here] + both[:, :, channels:]) + cbias_ref[...]
        line_ref[here] = done.astype(jnp.bfloat16)
        for r in range(block):
            row = jnp.minimum(first + block + 1 + r, height - 2)
            activate(mid_ref[row - 1], aff, keep, act_ref, row + 1)
        return 0

    lax.fori_loop(0, height // block, step, 0)
    out = pltpu.make_async_copy(line_ref, out_ref.at[1], sems.at[6])
    out.start()
    out.wait()


def far_kernel(block, flags_ref, edge_ref, mid_ref, top_ref, bottom_ref, aff_ref, x_ref, cbias_ref, acc0_ref, w_ref, old_ref,
               out_ref, act_ref, wk_ref, line_ref, sems):
    del old_ref
    height, width, channels = acc0_ref.shape
    copies = [pltpu.make_async_copy(w_ref.at[0, kh], wk_ref.at[kh], sems.at[kh]) for kh in range(TAPS)]
    for copy in copies:
        copy.start()
    aff = aff_ref[0:3]
    keep = flags_ref[0]
    activate(top_ref[...], aff, keep * flags_ref[1], act_ref, 0)
    activate(bottom_ref[...], aff, keep * flags_ref[2], act_ref, height + 1)
    activate(edge_ref[0], aff, keep, act_ref, 1)
    activate(edge_ref[1], aff, keep, act_ref, height)
    for r in range(1, block + 1):
        activate(mid_ref[r - 1], aff, keep, act_ref, r + 1)
    for copy in copies:
        copy.wait()

    def step(i, _):
        first = i * block
        part = row_dots(act_ref, first, block, lambda kh: wk_ref[kh]).reshape(block, width, channels)
        here = pl.ds(first, block)
        done = x_ref[here].astype(jnp.float32) + (acc0_ref[here] + part) + cbias_ref[...]
        line_ref[here] = done.astype(jnp.bfloat16)
        for r in range(block):
            row = jnp.minimum(first + block + 1 + r, height - 2)
            activate(mid_ref[row - 1], aff, keep, act_ref, row + 1)
        return 0

    lax.fori_loop(0, height // block, step, 0)
    out = pltpu.make_async_copy(line_ref, out_ref.at[0], sems.at[3])
    out.start()
    out.wait()


def shards(inputs, norm_gain, norm_bias, conv_weight, conv_bias):
    clips, frames, height, width, channels = inputs.shape
    assert clips == 1 and frames == TAPS - 1
    f32, bf16 = jnp.float32, jnp.bfloat16
    x = inputs.reshape(frames, height, width, channels)
    weight = conv_weight.reshape(TAPS, TAPS, TAPS * channels, channels)
    gain, bias, cbias = (v.reshape(1, channels) for v in (norm_gain, norm_bias, conv_bias))
    flags = jnp.stack([
        (lax.axis_index("tm") > 0).astype(jnp.int32),
        (lax.axis_index("rows") > 0).astype(jnp.int32),
        (lax.axis_index("rows") < lax.axis_size("rows") - 1).astype(jnp.int32),
    ])
    vmem = pl.BlockSpec(memory_space=pltpu.VMEM)
    smem = pl.BlockSpec(memory_space=pltpu.SMEM)
    hbm = pl.BlockSpec(memory_space=pl.ANY)
    params = pltpu.CompilerParams(vmem_limit_bytes=VMEM_LIMIT)
    block = 2
    shape = jax.ShapeDtypeStruct

    near_edge = ring(jnp.stack([x[1, 0], x[1, height - 1]]), "tm", 1)

    stats = pl.pallas_call(
        stats_kernel, out_shape=shape((2, channels), f32), in_specs=[vmem], out_specs=vmem,
        compiler_params=params, name="stats")(x.reshape(-1, width, channels))

    stats, count = merged(stats, "rows", 1.0 * frames * height * width)
    stats, count = merged(stats, "tm", count)

    own_top, own_bottom = row_halo(x[:, 0], x[:, height - 1], "rows")
    near_mid = ring(x[1, 1 : height - 1], "tm", 1)
    far_edge = ring(jnp.stack([x[0, 0], x[0, height - 1]]), "tm", 1)
    far_mid = ring(x[0, 1 : height - 1], "tm", 1)
    near_top, near_bottom = row_halo(near_edge[0], near_edge[1], "rows")
    far_top, far_bottom = row_halo(far_edge[0], far_edge[1], "rows")

    act = pltpu.VMEM((height + 2, width, TAPS * channels), bf16)
    wide = pltpu.VMEM((TAPS, TAPS * channels, 2 * channels), bf16)
    slim = pltpu.VMEM((TAPS, TAPS * channels, channels), bf16)
    line = pltpu.VMEM((height, width, channels), bf16)
    acc = shape((height, width, channels), f32)

    acc0, acc1, aff = pl.pallas_call(
        functools.partial(own_kernel, count, block),
        out_shape=(acc, acc, shape((8, channels), f32)),
        in_specs=[smem, vmem, vmem, vmem, vmem, vmem, vmem, hbm], out_specs=(vmem, vmem, vmem),
        scratch_shapes=[act, act, wide, slim, pltpu.SemaphoreType.DMA((9,))],
        compiler_params=params, name="own")(flags, x, own_top, own_bottom, stats, gain, bias, weight)

    acc0, out = pl.pallas_call(
        functools.partial(near_kernel, block),
        out_shape=(acc, shape((frames, height, width, channels), bf16)),
        in_specs=[smem] + [vmem] * 9 + [hbm], out_specs=(vmem, hbm),
        scratch_shapes=[act, wide, line, pltpu.SemaphoreType.DMA((7,))],
        compiler_params=params, name="near")(
            flags, near_edge, near_mid, near_top, near_bottom, aff, x[1], cbias, acc0, acc1, weight)

    out = pl.pallas_call(
        functools.partial(far_kernel, block),
        out_shape=shape((frames, height, width, channels), bf16),
        in_specs=[smem] + [vmem] * 8 + [hbm, hbm], out_specs=hbm,
        scratch_shapes=[act, slim, line, pltpu.SemaphoreType.DMA((4,))],
        input_output_aliases={10: 0},
        compiler_params=params, name="far")(
            flags, far_edge, far_mid, far_top, far_bottom, aff, x[0], cbias, acc0, weight, out)
    return out.reshape(inputs.shape)


def solution(mesh):
    placed = (P("batch", "tm", "rows", None, None), P(), P(), P(), P())
    return jax.shard_map(
        shards,
        mesh=mesh,
        in_specs=placed,
        out_specs=P("batch", "tm", "rows", None, None),
        check_vma=False,
    )
```

```python
import functools

import jax
import jax.numpy as jnp
from jax import lax
from jax.experimental import pallas as pl
from jax.experimental.pallas import tpu as pltpu
from jax.sharding import PartitionSpec as P


GROUPS = 32
epsilon = 1e-06
TAPS = 3
BLOCK = 2
MIB = 1024 * 1024


def ring(value, axis, step):
    count = lax.axis_size(axis)
    return lax.ppermute(value, axis, [(i, (i + step) % count) for i in range(count)])


def row_halo(first, last, axis, above):
    count = lax.axis_size(axis)
    if count == 1:
        return first, last
    if count == 2:
        both = ring(jnp.where(above == 0, last, first), axis, 1)
        return both, both
    return ring(last, axis, 1), ring(first, axis, -1)


def merged(stats, axis, step, count):
    size = lax.axis_size(axis)
    other = lax.ppermute(stats, axis, [(i, i ^ step) for i in range(size)])
    gap = stats[0:1] - other[0:1]
    second = lax.broadcasted_iota(jnp.int32, stats.shape, 0) == 1
    return stats + other + jnp.where(second, gap * gap * (0.5 / count), 0.0)


def prep_kernel(flags_ref, x_ref, w_ref, stats_ref, above_ref, keep_ref, w_all_ref, near_ref, edge_ref, far_ref, sems):
    frames, height, width, channels = keep_ref.shape
    fetch = pltpu.make_async_copy(x_ref, keep_ref, sems.at[0])
    fetch.start()
    copies = []
    for i, kt in enumerate((2, 1, 0)):
        copies.append(pltpu.make_async_copy(w_ref.at[kt], w_all_ref.at[:, pl.ds(i * channels, channels)], sems.at[1 + i]))
    for copy in copies:
        copy.start()
    fetch.wait()
    pieces = [
        pltpu.make_async_copy(keep_ref.at[1, pl.ds(1, height - 2)], near_ref, sems.at[4]),
        pltpu.make_async_copy(keep_ref.at[0, 0], edge_ref.at[0], sems.at[5]),
        pltpu.make_async_copy(keep_ref.at[0, height - 1], edge_ref.at[1], sems.at[6]),
        pltpu.make_async_copy(keep_ref.at[0, pl.ds(1, height - 2)], far_ref, sems.at[7]),
    ]
    for copy in pieces:
        copy.start()
    above_ref[...] = jnp.full(above_ref.shape, flags_ref[1], jnp.int32)
    per_step = 8
    steps = frames * height

    def tile(r):
        return keep_ref[r // height, r % height].astype(jnp.float32).reshape(-1, per_step, channels)

    def add(r, total):
        return total + jnp.sum(tile(r), axis=0)

    zeros = jnp.zeros((per_step, channels), jnp.float32)
    chan_sum = jnp.sum(lax.fori_loop(0, steps, add, zeros, unroll=2), axis=0, keepdims=True)
    mean = chan_sum * (1.0 / (steps * width))

    def square(r, total):
        gap = tile(r) - mean
        return total + jnp.sum(gap * gap, axis=0)

    stats_ref[0:1] = chan_sum
    stats_ref[1:2] = jnp.sum(lax.fori_loop(0, steps, square, zeros, unroll=2), axis=0, keepdims=True)
    for copy in copies + pieces:
        copy.wait()


def affine(stats_ref, gain_ref, bias_ref, aff_ref, count):
    channels = stats_ref.shape[-1]
    per_group = channels // GROUPS
    row = lax.broadcasted_iota(jnp.int32, (channels, channels), 0)
    col = lax.broadcasted_iota(jnp.int32, (channels, channels), 1)
    same = jnp.where(row // per_group == col // per_group, 1.0, 0.0)

    def group_mean(v):
        wide = jnp.broadcast_to(v, (8, channels))
        dot = jnp.dot(wide, same, precision=lax.Precision.HIGHEST, preferred_element_type=jnp.float32)
        return dot[0:1] * (1.0 / per_group)

    chan_mean = stats_ref[0:1] * (1.0 / count)
    mean = group_mean(chan_mean)
    gap = chan_mean - mean
    var = group_mean(stats_ref[1:2] * (1.0 / count) + gap * gap)
    aff_ref[0:1] = mean
    aff_ref[1:2] = lax.rsqrt(var + epsilon) * gain_ref[...].reshape(1, channels)
    aff_ref[2:3] = bias_ref[...].reshape(1, channels)


def activate(raw, aff, keep, act_ref, slot):
    width, channels = raw.shape
    normed = (raw.astype(jnp.float32) - aff[0:1]) * aff[1:2] + aff[2:3]
    active = normed * jax.nn.sigmoid(normed)
    if keep is not None:
        active = jnp.where(keep != 0, active, 0.0)
    place = lax.broadcasted_iota(jnp.int32, (width, channels), 0)
    before = jnp.where(place == 0, 0.0, pltpu.roll(active, 1, 0))
    after = jnp.where(place == width - 1, 0.0, pltpu.roll(active, width - 1, 0))
    act_ref[slot, :, 0:channels] = before.astype(jnp.bfloat16)
    act_ref[slot, :, channels : 2 * channels] = active.astype(jnp.bfloat16)
    act_ref[slot, :, 2 * channels : 3 * channels] = after.astype(jnp.bfloat16)


def taps(act_ref, first, rows):
    parts = []
    for kh in range(TAPS):
        part = act_ref[pl.ds(first + kh, rows)]
        parts.append(part.reshape(-1, part.shape[-1]))
    return jnp.concatenate(parts, axis=-1)


def own_kernel(count, flags_ref, x_ref, top_ref, bottom_ref, stats_ref, gain_ref, bias_ref, w_ref,
               acc0_ref, acc1_ref, aff_ref, act0_ref, act1_ref):
    _, height, width, channels = x_ref.shape
    steps = height // BLOCK
    affine(stats_ref, gain_ref, bias_ref, aff_ref, count)
    aff = aff_ref[0:3]

    def fill(f, slot, act_ref):
        if isinstance(slot, int):
            if slot == 0:
                return activate(top_ref[f], aff, flags_ref[1], act_ref, slot)
            if slot == height + 1:
                return activate(bottom_ref[f], aff, flags_ref[2], act_ref, slot)
            return activate(x_ref[f, slot - 1], aff, None, act_ref, slot)
        raw = jnp.where(slot == 0, top_ref[f], x_ref[f, jnp.clip(slot - 1, 0, height - 1)])
        raw = jnp.where(slot == height + 1, bottom_ref[f], raw)
        keep = jnp.where(slot == 0, flags_ref[1], jnp.where(slot == height + 1, flags_ref[2], 1))
        return activate(raw, aff, keep, act_ref, slot)

    for slot in range(BLOCK + 2):
        fill(0, slot, act0_ref)
    per_step = -(-(height + 2) // steps)

    def wide_step(i, _):
        first = i * BLOCK
        both = jnp.dot(taps(act0_ref, first, BLOCK), w_ref[:, 0 : 2 * channels], preferred_element_type=jnp.float32)
        acc0_ref[pl.ds(first, BLOCK)] = both[:, 0:channels].reshape(BLOCK, width, channels)
        acc1_ref[pl.ds(first, BLOCK)] = both[:, channels:].reshape(BLOCK, width, channels)
        for r in range(BLOCK):
            fill(0, jnp.minimum(first + BLOCK + 2 + r, height + 1), act0_ref)
        for r in range(per_step):
            fill(1, jnp.minimum(i * per_step + r, height + 1), act1_ref)
        return 0

    lax.fori_loop(0, steps, wide_step, 0)

    def slim_step(i, _):
        first = i * BLOCK
        last = jnp.dot(taps(act1_ref, first, BLOCK), w_ref[:, 0:channels], preferred_element_type=jnp.float32)
        here = pl.ds(first, BLOCK)
        acc1_ref[here] = acc1_ref[here] + last.reshape(BLOCK, width, channels)
        return 0

    lax.fori_loop(0, steps, slim_step, 0)


def halo_fill(flags_ref, edge_ref, mid_ref, top_ref, bottom_ref, aff, act_ref, slot):
    height = mid_ref.shape[0] + 2
    keep = flags_ref[0]
    if isinstance(slot, int):
        if slot == 0:
            return activate(top_ref[...], aff, keep * flags_ref[1], act_ref, slot)
        if slot == height + 1:
            return activate(bottom_ref[...], aff, keep * flags_ref[2], act_ref, slot)
        if slot == 1 or slot == height:
            return activate(edge_ref[int(slot == height)], aff, keep, act_ref, slot)
        return activate(mid_ref[slot - 2], aff, keep, act_ref, slot)
    raw = jnp.where(slot == height, edge_ref[1], mid_ref[jnp.clip(slot - 2, 0, height - 3)])
    raw = jnp.where(slot == height + 1, bottom_ref[...], raw)
    return activate(raw, aff, keep * jnp.where(slot == height + 1, flags_ref[2], 1), act_ref, slot)


def near_kernel(flags_ref, edge_ref, mid_ref, top_ref, bottom_ref, aff_ref, x_ref, cbias_ref, acc0_ref, acc1_ref, w_ref,
                new0_ref, out_ref, act_ref, line_ref, sems):
    height, width, channels = acc0_ref.shape
    aff = aff_ref[0:3]
    cbias = cbias_ref[...].reshape(1, channels)
    fill = functools.partial(halo_fill, flags_ref, edge_ref, mid_ref, top_ref, bottom_ref, aff, act_ref)
    for slot in range(BLOCK + 2):
        fill(slot)

    def copy_out(i):
        here = pl.ds(i * BLOCK, BLOCK)
        return pltpu.make_async_copy(line_ref.at[here], out_ref.at[1, here], sems.at[i])

    def step(i, _):
        first = i * BLOCK
        both = jnp.dot(taps(act_ref, first, BLOCK), w_ref[:, channels:], preferred_element_type=jnp.float32)
        both = both.reshape(BLOCK, width, 2 * channels)
        here = pl.ds(first, BLOCK)
        new0_ref[here] = acc0_ref[here] + both[:, :, 0:channels]
        done = x_ref[1, here].astype(jnp.float32) + (acc1_ref[here] + both[:, :, channels:]) + cbias
        line_ref[here] = done.astype(jnp.bfloat16)
        for r in range(BLOCK):
            fill(jnp.minimum(first + BLOCK + 2 + r, height + 1))
        copy_out(i).start()
        return 0

    lax.fori_loop(0, height // BLOCK, step, 0)
    for i in range(height // BLOCK):
        copy_out(i).wait()


def far_kernel(flags_ref, edge_ref, mid_ref, top_ref, bottom_ref, aff_ref, x_ref, cbias_ref, acc0_ref, w_ref, old_ref,
               out_ref, act_ref, line_ref, sems):
    del old_ref
    height, width, channels = acc0_ref.shape
    aff = aff_ref[0:3]
    cbias = cbias_ref[...].reshape(1, channels)
    fill = functools.partial(halo_fill, flags_ref, edge_ref, mid_ref, top_ref, bottom_ref, aff, act_ref)
    for slot in range(BLOCK + 2):
        fill(slot)

    def copy_out(i):
        here = pl.ds(i * BLOCK, BLOCK)
        return pltpu.make_async_copy(line_ref.at[here], out_ref.at[0, here], sems.at[i])

    def step(i, _):
        first = i * BLOCK
        part = jnp.dot(taps(act_ref, first, BLOCK), w_ref[:, 2 * channels :], preferred_element_type=jnp.float32)
        here = pl.ds(first, BLOCK)
        done = x_ref[0, here].astype(jnp.float32) + (acc0_ref[here] + part.reshape(BLOCK, width, channels)) + cbias
        line_ref[here] = done.astype(jnp.bfloat16)
        for r in range(BLOCK):
            fill(jnp.minimum(first + BLOCK + 2 + r, height + 1))
        copy_out(i).start()
        return 0

    lax.fori_loop(0, height // BLOCK, step, 0)
    for i in range(height // BLOCK):
        copy_out(i).wait()


def shards(inputs, norm_gain, norm_bias, conv_weight, conv_bias):
    clips, frames, height, width, channels = inputs.shape
    assert clips == 1 and frames == TAPS - 1 and height % BLOCK == 0
    f32, bf16 = jnp.float32, jnp.bfloat16
    x = inputs.reshape(frames, height, width, channels)
    weight = conv_weight.reshape(TAPS, TAPS * TAPS * channels, channels)
    flags = jnp.stack([
        (lax.axis_index("tm") > 0).astype(jnp.int32),
        (lax.axis_index("rows") > 0).astype(jnp.int32),
        (lax.axis_index("rows") < lax.axis_size("rows") - 1).astype(jnp.int32),
    ])
    vmem = pl.BlockSpec(memory_space=pltpu.VMEM)
    smem = pl.BlockSpec(memory_space=pltpu.SMEM)
    hbm = pl.BlockSpec(memory_space=pltpu.HBM)
    shape = jax.ShapeDtypeStruct
    dma = pltpu.SemaphoreType.DMA

    def params(mib):
        return pltpu.CompilerParams(vmem_limit_bytes=mib * MIB)

    near_edge = ring(x[1, :: height - 1], "tm", 1)
    stats, above, kept, w_all, near_src, far_edge_src, far_src = pl.pallas_call(
        prep_kernel,
        out_shape=(
            shape((2, channels), f32), shape((channels,), jnp.int32), pltpu.VMEM(x.shape, bf16),
            pltpu.VMEM((weight.shape[1], TAPS * channels), bf16), shape((height - 2, width, channels), bf16),
            shape((2, width, channels), bf16), shape((height - 2, width, channels), bf16)),
        in_specs=[smem, hbm, hbm], out_specs=(vmem, vmem, vmem, vmem, hbm, hbm, hbm), scratch_shapes=[dma((8,))],
        compiler_params=params(2), name="prep")(
            flags, pltpu.with_memory_space_constraint(x, pltpu.HBM), pltpu.with_memory_space_constraint(weight, pltpu.HBM))

    kept, w_all = (pltpu.with_memory_space_constraint(v, pltpu.VMEM) for v in (kept, w_all))
    count = 1.0 * frames * height * width
    step = 1
    while step < lax.axis_size("rows"):
        stats = merged(stats, "rows", step, count)
        count, step = 2.0 * count, 2 * step
    step = 1
    while step < lax.axis_size("tm"):
        stats = merged(stats, "tm", step, count)
        count, step = 2.0 * count, 2 * step

    own_top, own_bottom = row_halo(x[:, 0], x[:, height - 1], "rows", above)
    near_mid = ring(near_src, "tm", 1)
    far_edge = ring(far_edge_src, "tm", 1)
    far_mid = ring(far_src, "tm", 1)
    near_top, near_bottom = row_halo(near_edge[0], near_edge[1], "rows", above)
    far_top, far_bottom = row_halo(far_edge[0], far_edge[1], "rows", above)

    act = pltpu.VMEM((height + 2, width, TAPS * channels), bf16)
    line = pltpu.VMEM((height, width, channels), bf16)
    acc = pltpu.VMEM((height, width, channels), f32)

    acc0, acc1, aff = pl.pallas_call(
        functools.partial(own_kernel, count),
        out_shape=(acc, acc, pltpu.VMEM((8, channels), f32)),
        in_specs=[smem] + [vmem] * 7, out_specs=(vmem, vmem, vmem),
        scratch_shapes=[act, act],
        compiler_params=params(12), name="own")(
            flags, kept, own_top, own_bottom, stats, norm_gain, norm_bias, w_all)

    acc0, out = pl.pallas_call(
        near_kernel,
        out_shape=(acc, shape((frames, height, width, channels), bf16)),
        in_specs=[smem] + [vmem] * 10, out_specs=(vmem, hbm),
        scratch_shapes=[act, line, dma((height // BLOCK,))],
        compiler_params=params(8), name="near")(
            flags, near_edge, near_mid, near_top, near_bottom, aff, kept, conv_bias, acc0, acc1, w_all)

    out = pl.pallas_call(
        far_kernel,
        out_shape=shape((frames, height, width, channels), bf16),
        in_specs=[smem] + [vmem] * 9 + [hbm], out_specs=hbm,
        scratch_shapes=[act, line, dma((height // BLOCK,))],
        input_output_aliases={10: 0},
        compiler_params=params(8), name="far")(
            flags, far_edge, far_mid, far_top, far_bottom, aff, kept, conv_bias, acc0, w_all, out)
    return out.reshape(inputs.shape)


def solution(mesh):
    placed = (P("batch", "tm", "rows", None, None), P(), P(), P(), P())
    return jax.shard_map(
        shards,
        mesh=mesh,
        in_specs=placed,
        out_specs=P("batch", "tm", "rows", None, None),
        check_vma=False,
    )
```
